32 devices in a mesh: rep: 2 (over x), dp: 16 (over y, z, core).
Axes of the slice: x: 2, y: 2, z: 4, core: 2. Of those that a mesh axis runs over, the one named last changes fastest.
Arguments:
- x: bfloat16 [32, 2048, 1024], P(('rep', 'dp')), parts along dimension 0
- dy: bfloat16 [32, 2048, 1024], P(('rep', 'dp')), parts along dimension 0
- w_gate: bfloat16 [2, 1024, 3200], P(None, 'dp')
- w_up: bfloat16 [2, 1024, 3200], P(None, 'dp')
- w_down: bfloat16 [2, 3200, 1024], P(None, 'dp')
- m_w_gate: float32 [2, 1024, 3200], P(None, 'dp')
- m_w_up: float32 [2, 1024, 3200], P(None, 'dp')
- m_w_down: float32 [2, 3200, 1024], P(None, 'dp')
- v_w_gate: float32 [2, 1024, 3200], P(None, 'dp')
- v_w_up: float32 [2, 1024, 3200], P(None, 'dp')
- v_w_down: float32 [2, 3200, 1024], P(None, 'dp')
Outputs:
- output 1: bfloat16 [4, 1024, 3200], P('rep', 'dp'), parts along dimension 0
- output 2: bfloat16 [4, 1024, 3200], P('rep', 'dp'), parts along dimension 0
- output 3: bfloat16 [4, 3200, 1024], P('rep', 'dp'), parts along dimension 0
- output 4: float32 [4, 1024, 3200], P('rep', 'dp'), parts along dimension 0
- output 5: float32 [4, 1024, 3200], P('rep', 'dp'), parts along dimension 0
- output 6: float32 [4, 3200, 1024], P('rep', 'dp'), parts along dimension 0
- output 7: float32 [4, 1024, 3200], P('rep', 'dp'), parts along dimension 0
- output 8: float32 [4, 1024, 3200], P('rep', 'dp'), parts along dimension 0
- output 9: float32 [4, 3200, 1024], P('rep', 'dp'), parts along dimension 0
There are 2 independent parts. The reference program is written for one: setup_inputs(seed, part) draws one part's arguments, and reference() takes and returns one part's arrays. A program takes and returns all parts, laid end to end along the dimension named above; an argument that names none is the same for every part.
All inputs are finite; a program needn't handle non-finite values.
Results may differ from the reference program's by a relative error of at most 0.022.
Values are sent between devices in bfloat16 or wider.
A program may use at most 2 GiB of HBM per device.

```python
import jax
import jax.numpy as jnp
from jax import lax

SEQUENCES = 16
TOKENS = 2048
D = 1024
FF = 3200
LAYERS = 2
NAMES = ("w_gate", "w_up", "w_down")
SHAPES = {"w_gate": (LAYERS, D, FF), "w_up": (LAYERS, D, FF), "w_down": (LAYERS, FF, D)}


def bump(key, n, height):
    away = (jnp.arange(n, dtype=jnp.int32) - jax.random.randint(key, (), 0, n, jnp.int32)) % n
    return jnp.where(away < n // 8, height, 1.0)


def together(key, own, strength):
    shared = jax.random.normal(key, own.shape[1:], jnp.float32)
    return (own + strength * shared) * lax.rsqrt(1 + strength * strength)


def setup_inputs(seed: int = 0, part: int = 0) -> dict:
    kx, kdy, ka, kb, kz, kf, kh, kl, *keys = jax.random.split(jax.random.key(seed), 8 + 3 * len(NAMES))
    kx, kdy, ka, kb = (jax.random.fold_in(k, part) for k in (kx, kdy, ka, kb))
    kw, km, kv = (keys[i::3] for i in range(3))
    shape = (SEQUENCES, TOKENS, D)
    much_x, much_dy = jax.random.uniform(kz, (2,), jnp.float32, 0.0, 1.0)
    loud = 2.0 ** jax.random.uniform(jax.random.fold_in(kz, 1), (), jnp.float32, -1.0, 2.0)
    layers = 2.0 ** jax.random.uniform(kl, (LAYERS, 1, 1), jnp.float32, -1.0, 1.0)
    x = together(ka, jax.random.normal(kx, shape, jnp.float32), much_x) * bump(kf, D, 4.0)
    dy = together(kb, jax.random.normal(kdy, shape, jnp.float32), much_dy)
    drawn = {"x": x.astype(jnp.bfloat16), "dy": (loud * dy * (SEQUENCES * TOKENS) ** -0.5).astype(jnp.bfloat16)}
    for key, name in zip(kw, NAMES, strict=True):
        w = jax.random.normal(key, SHAPES[name], jnp.float32) * SHAPES[name][1] ** -0.5
        drawn[name] = (w * {"w_gate": 1.0, "w_up": bump(kh, FF, 4.0), "w_down": layers}[name]).astype(jnp.bfloat16)
    for key, name in zip(km, NAMES, strict=True):
        drawn[f"m_{name}"] = 0.1 * jax.random.normal(key, SHAPES[name], jnp.float32)
    for key, name in zip(kv, NAMES, strict=True):
        drawn[f"v_{name}"] = jax.random.uniform(key, SHAPES[name], jnp.float32, 0.005, 0.015)
    return drawn


def matmul(a, w):
    return jnp.dot(a, w, preferred_element_type=jnp.float32).astype(jnp.bfloat16)


def normed(h):
    wide = h.astype(jnp.float32)
    scale = lax.rsqrt(jnp.mean(wide**2, -1, keepdims=True) + 1e-6)
    return (wide * scale).astype(jnp.bfloat16)


def layer(h, w):
    a = normed(h)
    gate = jnp.dot(a, w["w_gate"], preferred_element_type=jnp.float32)
    up = jnp.dot(a, w["w_up"], preferred_element_type=jnp.float32)
    return h + matmul((jax.nn.silu(gate) * up).astype(jnp.bfloat16), w["w_down"])


def adamw(w, m, v, g):
    m = 0.9 * m + 0.1 * g
    v = 0.95 * v + 0.05 * g * g
    step = m * lax.rsqrt(v + 1e-8) + 0.1 * w
    return (w - 0.02 * step).astype(jnp.bfloat16), m, v


def stack(weights, h):
    return lax.scan(lambda h, w: (layer(h, w), None), h, weights)[0]


def reference(x, dy, w_gate, w_up, w_down, m_w_gate, m_w_up, m_w_down, v_w_gate, v_w_up, v_w_down):
    weights = dict(zip(NAMES, (w_gate, w_up, w_down), strict=True))

    def take(so_far, sequence):
        h, by_y = sequence
        _, back = jax.vjp(lambda w: stack(w, h), weights)
        return jax.tree.map(lambda total, term: total + term.astype(jnp.float32), so_far, back(by_y)[0]), None

    none_yet = {name: jnp.zeros(w.shape, jnp.float32) for name, w in weights.items()}
    by_weights, _ = lax.scan(take, none_yet, (x, dy))
    gradients = [by_weights[name].astype(jnp.bfloat16).astype(jnp.float32) for name in NAMES]
    new = [
        adamw(w.astype(jnp.float32), m, v, g)
        for w, m, v, g in zip((w_gate, w_up, w_down), (m_w_gate, m_w_up, m_w_down), (v_w_gate, v_w_up, v_w_down), gradients, strict=True)
    ]
    return tuple(one[which] for which in range(3) for one in new)
```

```python
import functools

import jax
import jax.numpy as jnp
from jax import lax
from jax.experimental import pallas as pl
from jax.experimental.pallas import tpu as pltpu
from jax.sharding import PartitionSpec as P

NAMES = ("w_gate", "w_up", "w_down")
BF, WIDE = jnp.bfloat16, jnp.float32
MESH = pl.DeviceIdType.MESH
ANY = pl.BlockSpec(memory_space=pl.ANY)
VMEM = pltpu.VMEM
ROOM = 66_000_000
T, D, FF = 2048, 1024, 3200
RG, RD, PAD = D // 16, FF // 16, 208
TILE = 256
CHUNKS = ((0, 1024), (1024, 1024), (2048, 1152))


def adamw(w, m, v, g):
    m = 0.9 * m + 0.1 * g
    v = 0.95 * v + 0.05 * g * g
    step = m * lax.rsqrt(v + 1e-8) + 0.1 * w
    return (w - 0.02 * step).astype(BF), m, v


def dot(a, b, dims=((1,), (0,))):
    return lax.dot_general(a, b, (dims, ((), ())), preferred_element_type=WIDE)


def place():
    me = lax.axis_index("dp")
    return me // 8, me // 2 % 4, me % 2, lax.axis_index("rep")


def number(y, z, c):
    return (y * 4 + z) * 2 + c


def flip(bit):
    return 1 - bit


def xor4(z, k):
    low, high = z % 2, z // 2
    low = 1 - low if k % 2 else low
    high = 1 - high if k // 2 else high
    return high * 2 + low


def meet(barrier):
    y, z, c, x = place()
    peers = [{"dp": number(y, xor4(z, k), c)} for k in (1, 2, 3)]
    peers += [{"dp": number(1 - y, z, c)}, {"dp": number(y, z, 1 - c)}]
    return peers


def norm_scale(wide):
    return lax.rsqrt(jnp.mean(wide * wide, -1, keepdims=True) + 1e-6)


def put_hidden(hid_t, out):
    for i in range(16):
        out[i, 0:RD, :] = hid_t[i * RD : (i + 1) * RD, :].astype(BF)
        out[i, RD:PAD, :] = jnp.zeros((PAD - RD, TILE), BF)


class Gather:
    def __init__(self, base, layer, gu, wd, full, down, send, recv):
        self.y, self.z, self.c, self.x = place()
        self.layer, self.gu, self.wd, self.full, self.down, self.send, self.recv = layer, gu, wd, full, down, send, recv
        self.base = base

    def at(self, dy, k):
        return number(flip(self.y) if dy else self.y, xor4(self.z, k), self.c)

    def copy(self, which, stage, dy, k):
        kinds = ("Az", "Dz", "Ay", "Dy", "Ox", "Ac", "Oc", "Dc")
        sem = self.base + kinds.index(which + stage) * 8 + dy * 4 + k
        peer = {
            "z": lambda: {"dp": number(self.y, xor4(self.z, k), self.c)},
            "y": lambda: {"dp": number(1 - self.y, self.z, self.c)},
            "c": lambda: {"dp": number(self.y, self.z, 1 - self.c)},
            "x": lambda: {"rep": 1 - self.x},
        }[stage]()
        own = stage == "z" or (dy == 0 and k == 0)
        b = self.at(0, 0) if own else self.at(dy, k)
        if which == "D":
            dst = self.down.at[pl.ds(b * RD, RD), :]
            src = self.wd.at[self.layer] if own else dst
        else:
            m = 1 - self.x if which == "O" and stage == "c" else self.x
            dst = self.full.at[m, b]
            src = self.gu.at[m, self.layer] if own else dst
        return pltpu.make_async_remote_copy(
            src_ref=src, dst_ref=dst, send_sem=self.send.at[sem], recv_sem=self.recv.at[sem], device_id=peer, device_id_type=MESH
        )

    def begin(self):
        for k in (1, 2, 3):
            self.copy("A", "z", 0, k).start()
        self.copy("A", "y", 0, 0).start()
        for k in (1, 2, 3):
            self.copy("D", "z", 0, k).start()
        self.copy("D", "y", 0, 0).start()
        for which in "AOD":
            self.copy(which, "c", 0, 0).start()

    def passed_on(self, event):
        which, stage, dy, k = event
        self.copy(which, stage, dy, k).wait_recv()
        if stage == "z":
            self.copy(which, "y", 0, k).start()
            self.copy(which, "c", 0, k).start()
            if which == "A":
                self.copy("O", "x", 0, k).start()
        elif stage == "y":
            self.copy(which, "c", 1, k).start()
            if which == "A":
                self.copy("O", "x", 1, k).start()
        elif stage == "x":
            self.copy("O", "c", dy, k).start()

    EVENTS = ("Az01", "Az02", "Az03", "Ay00", "Ay01", "Ox01", "Dz01", "Ay02", "Ox02", "Dz02", "Ay03")
    EVENTS += ("Ox03", "Dz03", "Ox10", "Dy00", "Dy01", "Ox11", "Dy02", "Ox12", "Dy03", "Ox13")

    @staticmethod
    def parse(e):
        return e[0], e[1], int(e[2]), int(e[3])

    def all_core(self):
        for which in "AOD":
            for dy in range(2):
                for k in range(4):
                    self.copy(which, "c", dy, k).wait_recv()

    def all_sent(self):
        for which in "AD":
            for k in (1, 2, 3):
                self.copy(which, "z", 0, k).wait_send()
            for k in range(4):
                self.copy(which, "y", 0, k).wait_send()
        for dy in range(2):
            for k in range(4):
                if dy or k:
                    self.copy("O", "x", dy, k).wait_send()
                for which in "AOD":
                    self.copy(which, "c", dy, k).wait_send()


def forward_kernel(
    gu, wd, x, full0, down0, full1, down1, gate_out, up_out, hid_out, a_out, h_out,
    wg_s, wu_s, wd_s, hid_s, own_gu, own_d, send, recv, local,
):
    i = pl.program_id(0)
    steps = T // TILE
    y, z, c, xx = place()
    g0 = Gather(0, 0, gu, wd, full0, down0, send, recv)
    g1 = Gather(64, 1, gu, wd, full1, down1, send, recv)

    @pl.when(i == 0)
    def _():
        barrier = pltpu.get_barrier_semaphore()
        peers = meet(barrier) + [{"rep": 1 - xx}]
        for peer in peers:
            pl.semaphore_signal(barrier, inc=1, device_id=peer, device_id_type=MESH)
        pl.semaphore_wait(barrier, len(peers))
        g0.begin()
        ins = [pltpu.make_async_copy(gu, own_gu, local.at[0]), pltpu.make_async_copy(wd, own_d, local.at[1])]
        for one in ins:
            one.start()
        for one in ins:
            one.wait()
        me = number(y, z, c)
        outs = []
        for l, (full, down) in enumerate(((full0, down0), (full1, down1))):
            for m in range(2):
                outs.append(pltpu.make_async_copy(own_gu.at[m, l], full.at[m, me], local.at[2 + 3 * l + m]))
            outs.append(pltpu.make_async_copy(own_d.at[l], down.at[pl.ds(me * RD, RD), :], local.at[4 + 3 * l]))
        for one in outs:
            one.start()
        for e in Gather.EVENTS:
            g0.passed_on(Gather.parse(e))
            if e == "Dz03":
                g1.begin()
        for one in outs:
            one.wait()
        g0.all_core()
        loads = [
            pltpu.make_async_copy(full0.at[0], wg_s, local.at[0]),
            pltpu.make_async_copy(full0.at[1], wu_s, local.at[1]),
            pltpu.make_async_copy(down0, wd_s, local.at[2]),
        ]
        for one in loads:
            one.start()
        for one in loads:
            one.wait()

    wide = x[...].astype(WIDE)
    a_wide = (wide * norm_scale(wide)).astype(BF)
    a_out[...] = jnp.swapaxes(a_wide.astype(WIDE), 0, 1).astype(BF)

    total = jnp.zeros((TILE, D), WIDE)
    for at, size in CHUNKS:
        gate = dot(a_wide, wg_s[:, :, at : at + size].reshape(D, size))
        up = dot(a_wide, wu_s[:, :, at : at + size].reshape(D, size))
        gate_out[:, at : at + size] = gate
        up_out[:, at : at + size] = up
        hid = gate * (1.0 / (1.0 + jnp.exp(-gate))) * up
        hid_s[at : at + size, :] = jnp.swapaxes(hid, 0, 1)
        total = total + dot(hid.astype(BF), wd_s[at : at + size, :])
    put_hidden(hid_s, hid_out)
    h_out[...] = (wide + total.astype(BF).astype(WIDE)).astype(BF)

    for t in range(steps):
        mine = Gather.EVENTS[t * 3 : t * 3 + 3]

        @pl.when(i == t)
        def _():
            for e in mine:
                g1.passed_on(Gather.parse(e))
            if t == steps - 1:
                g1.all_core()
                g0.all_sent()
                g1.all_sent()


def forward(x, w_gate, w_up, w_down):
    steps = T // TILE
    gu = jnp.stack([w_gate, w_up])
    full = jax.ShapeDtypeStruct((2, 16, RG, FF), BF)
    down = jax.ShapeDtypeStruct((FF, D), BF)
    rows = lambda n: pl.BlockSpec((TILE, n), lambda i: (i, 0))
    return pl.pallas_call(
        forward_kernel,
        grid=(steps,),
        in_specs=[ANY, ANY, rows(D)],
        out_specs=[ANY] * 4
        + [rows(FF), rows(FF), pl.BlockSpec((16, PAD, TILE), lambda i: (0, 0, i)), pl.BlockSpec((D, TILE), lambda i: (0, i)), rows(D)],
        out_shape=[full, down, full, down]
        + [jax.ShapeDtypeStruct((T, FF), WIDE)] * 2
        + [jax.ShapeDtypeStruct((16, PAD, T), BF), jax.ShapeDtypeStruct((D, T), BF), jax.ShapeDtypeStruct((T, D), BF)],
        scratch_shapes=[
            VMEM((16, RG, FF), BF),
            VMEM((16, RG, FF), BF),
            VMEM((FF, D), BF),
            VMEM((FF, TILE), WIDE),
            VMEM((2, 2, RG, FF), BF),
            VMEM((2, RD, D), BF),
            pltpu.SemaphoreType.DMA((128,)),
            pltpu.SemaphoreType.DMA((128,)),
            pltpu.SemaphoreType.DMA((8,)),
        ],
        compiler_params=pltpu.CompilerParams(
            collective_id=0, has_side_effects=True, vmem_limit_bytes=ROOM, dimension_semantics=("arbitrary",)
        ),
        name="forward",
    )(gu, w_down, x)


def turn_kernel(h, dy, gu, wd, hid_out, a_out, dg_out, du_out, hid_s):
    wide = h[...].astype(WIDE)
    a = (wide * norm_scale(wide)).astype(BF)
    a_out[...] = jnp.swapaxes(a.astype(WIDE), 0, 1).astype(BF)
    for at, size in CHUNKS:
        gate = dot(a, gu[0, :, at : at + size])
        up = dot(a, gu[1, :, at : at + size])
        back = dot(dy[...], wd[at : at + size, :], ((1,), (1,))).astype(BF).astype(WIDE)
        sig = 1.0 / (1.0 + jnp.exp(-gate))
        act = gate * sig
        hid_s[at : at + size, :] = jnp.swapaxes(act * up, 0, 1)
        du_out[:, at : at + size] = (back * act).astype(BF)
        dg_out[:, at : at + size] = (back * up * (sig + act * (1.0 - sig))).astype(BF)
    put_hidden(hid_s, hid_out)


def once(shape):
    return pl.BlockSpec(shape, lambda i: (0,) * len(shape), pipeline_mode=pl.Buffered(1))


def turn(h, dy, full, down):
    rows = lambda n: pl.BlockSpec((TILE, n), lambda i: (i, 0))
    return pl.pallas_call(
        turn_kernel,
        grid=(T // TILE,),
        in_specs=[rows(D), rows(D), once((2, D, FF)), once((FF, D))],
        out_specs=[pl.BlockSpec((16, PAD, TILE), lambda i: (0, 0, i)), pl.BlockSpec((D, TILE), lambda i: (0, i)), rows(FF), rows(FF)],
        out_shape=[jax.ShapeDtypeStruct((16, PAD, T), BF), jax.ShapeDtypeStruct((D, T), BF)] + [jax.ShapeDtypeStruct((T, FF), BF)] * 2,
        scratch_shapes=[VMEM((FF, TILE), WIDE)],
        compiler_params=pltpu.CompilerParams(vmem_limit_bytes=ROOM, dimension_semantics=("arbitrary",)),
        name="turn",
    )(h, dy, full.reshape(2, D, FF), down)


def back_tile(dg, du, h, dy, gu, out):
    da = dot(dg, gu[0], ((1,), (1,))).astype(BF).astype(WIDE) + dot(du, gu[1], ((1,), (1,))).astype(BF).astype(WIDE)
    da = da.astype(BF).astype(WIDE)
    wide = h.astype(WIDE)
    scale = norm_scale(wide)
    along = jnp.sum(da * wide, -1, keepdims=True)
    by_h = da * scale - wide * (scale * scale * scale * along * (1.0 / D))
    out[...] = (dy.astype(WIDE) + by_h.astype(BF).astype(WIDE)).astype(BF)


def through_tile(dy, gate_in, up_in, wd, dg_out, du_out):
    for at, size in CHUNKS:
        gate, up = gate_in[:, at : at + size], up_in[:, at : at + size]
        back = dot(dy[...], wd[at : at + size, :], ((1,), (1,))).astype(BF).astype(WIDE)
        sig = 1.0 / (1.0 + jnp.exp(-gate))
        act = gate * sig
        du_out[:, at : at + size] = (back * act).astype(BF)
        dg_out[:, at : at + size] = (back * up * (sig + act * (1.0 - sig))).astype(BF)


ORDER = (3, 2, 1, 0)


AFTER_PRODUCT = {3: (0,), 5: (1,), 7: (2,), 9: (4,), 10: (3,), 11: (5,)}
AFTER_BACK = {0: (6,), 4: (8,), 5: (7,), 7: (9,)}
AFTER_THROUGH = {0: (10,), 5: (11,)}


def scatter_kernel(more, *refs):
    hid, a, dy, dg, du = refs[:5]
    refs = refs[5:]
    if more:
        h, gu, wd, gate, up = refs[:5]
        refs = refs[5:]
    gg_out, gu_out, gd_out = refs[:3]
    refs = refs[3:]
    if more:
        dh_out, dg_out, du_out = refs[:3]
        refs = refs[3:]
    own, own_d, r1, r1_d, cs, cs_d, r2, r2_d, r3, r3_d, send, recv, local, tiled = refs
    y, z, c, _ = place()
    barrier = pltpu.get_barrier_semaphore()
    peers = meet(barrier)
    for peer in peers:
        pl.semaphore_signal(barrier, inc=1, device_id=peer, device_id_type=MESH)

    def bufs(s):
        m, k = s // 4, ORDER[s % 4]
        if m == 0:
            return own_d.at[k], r1_d.at[k], cs_d.at[s % 2], r2_d.at[k], (r3_d.at[k - 1] if k else None)
        j = (m - 1) * 4 + k
        return own.at[j], r1.at[j], cs.at[s % 2], r2.at[j], (r3.at[(m - 1) * 3 + k - 1] if k else None)

    def remote(src, dst, sem, peer):
        return pltpu.make_async_remote_copy(
            src_ref=src, dst_ref=dst, send_sem=send.at[sem], recv_sem=recv.at[sem], device_id=peer, device_id_type=MESH
        )

    def by_core(s):
        _, one, out, _, _ = bufs(s)
        return remote(out, one, s, {"dp": number(y, z, 1 - c)})

    def by_y(s):
        mine, _, _, two, _ = bufs(s)
        return remote(mine.at[1], two, 12 + s, {"dp": number(1 - y, z, c)})

    def by_z(s):
        mine, _, _, _, three = bufs(s)
        return remote(mine.at[0], three, 24 + s, {"dp": number(y, xor4(z, ORDER[s % 4]), c)})

    def lhs_copies(s, lhs, lhs_d):
        m, k = s // 4, ORDER[s % 4]
        src, dst = (hid, lhs_d) if m == 0 else (a, lhs)
        out = []
        for dy_ in range(2):
            for dc in range(2):
                b = number(flip(y) if dy_ else y, xor4(z, k), flip(c) if dc else c)
                sem = 4 * (s % 2) + dy_ * 2 + dc
                rows = PAD if m == 0 else RG
                out.append(pltpu.make_async_copy(src.at[b], dst.at[s % 2, pl.ds((dy_ * 2 + dc) * rows, rows), :], local.at[sem]))
        return out

    def widths(m):
        return (256, 4) if m == 0 else (640, 5)

    def product(s, left, right):
        m = s // 4
        rows, r = (PAD, RD) if m == 0 else (RG, RG)
        mine, _, out, _, _ = bufs(s)
        size, n = widths(m)

        def body(j, _):
            cols = pl.ds(pl.multiple_of(j * size, size), size)
            p = dot(left[s % 2], right[:, cols])
            for dy_ in range(2):
                mine[dy_, :, cols] = p[(dy_ * 2) * rows : (dy_ * 2) * rows + r].astype(BF)
                out[dy_, :, cols] = p[(dy_ * 2 + 1) * rows : (dy_ * 2 + 1) * rows + r].astype(BF)
            return 0

        lax.fori_loop(0, n, body, 0)

    def each(m, fn):
        size, n = widths(m)

        def body(j, _):
            fn(pl.ds(pl.multiple_of(j * size, size), size))
            return 0

        lax.fori_loop(0, n, body, 0)

    def to_y(s):
        mine, one, _, _, _ = bufs(s)
        by_core(s).wait_recv()

        def fn(cols):
            mine[1, :, cols] = (mine[1, :, cols].astype(WIDE) + one[1, :, cols].astype(WIDE)).astype(BF)

        each(s // 4, fn)
        by_y(s).start()

    def to_z(s):
        m, k = s // 4, ORDER[s % 4]
        mine, one, _, two, _ = bufs(s)
        by_y(s).wait_recv()
        if k:

            def fn(cols):
                mine[0, :, cols] = (
                    mine[0, :, cols].astype(WIDE) + one[0, :, cols].astype(WIDE) + two[:, cols].astype(WIDE)
                ).astype(BF)

            each(m, fn)
            by_z(s).start()
            return
        threes = []
        for t in range(4 * m, 4 * m + 3):
            by_z(t).wait_recv()
            threes.append(bufs(t)[4])
        result = (gd_out, gg_out, gu_out)[m]

        def fn(cols):
            total = mine[0, :, cols].astype(WIDE) + one[0, :, cols].astype(WIDE) + two[:, cols].astype(WIDE)
            for three in threes:
                total = total + three[:, cols].astype(WIDE)
            result[:, cols] = total.astype(BF)

        each(m, fn)

    def products(rhs, rhs_d, lhs, lhs_d):
        right_d = pltpu.make_async_copy(dy, rhs_d, local.at[8])
        right_g = pltpu.make_async_copy(dg, rhs, local.at[9])
        right_u = pltpu.make_async_copy(du, rhs, local.at[9])
        for one in lhs_copies(0, lhs, lhs_d):
            one.start()
        right_d.start()
        right_g.start()
        pl.semaphore_wait(barrier, len(peers))
        for s in range(12):
            for one in lhs_copies(s, lhs, lhs_d):
                one.wait()
            if s + 1 < 12:
                for one in lhs_copies(s + 1, lhs, lhs_d):
                    one.start()
            if s == 0:
                right_d.wait()
            if s == 4:
                right_g.wait()
            if s == 8:
                right_u.wait()
            if s >= 2:
                by_core(s - 2).wait_send()
            product(s, lhs_d if s < 4 else lhs, rhs_d if s < 4 else rhs)
            if s == 7:
                right_u.start()
            by_core(s).start()
            if s >= 1:
                to_y(s - 1)
            for q in AFTER_PRODUCT.get(s, ()):
                to_z(q)

    def tiles(ins, outs, compute, after):
        n = T // TILE

        def copies(pairs, j, base, inward):
            out = []
            for i, (far, near) in enumerate(pairs):
                rows = far.at[pl.ds(pl.multiple_of(j * TILE, TILE), TILE), :]
                slot = near.at[j % 2]
                sem = tiled.at[base + 2 * i + j % 2]
                out.append(pltpu.make_async_copy(rows, slot, sem) if inward else pltpu.make_async_copy(slot, rows, sem))
            return out

        for one in copies(ins, 0, 0, True):
            one.start()

        def body(j, _):
            @pl.when(j + 1 < n)
            def _():
                for one in copies(ins, j + 1, 0, True):
                    one.start()

            for one in copies(ins, j, 0, True):
                one.wait()

            @pl.when(j >= 2)
            def _():
                for one in copies(outs, j - 2, 10, False):
                    one.wait()

            compute(j % 2)
            for one in copies(outs, j, 10, False):
                one.start()
            for t, which in after.items():

                @pl.when(j == t)
                def _():
                    for q in which:
                        to_z(q)

            return 0

        lax.fori_loop(0, n, body, 0)
        for j in (n - 2, n - 1):
            for one in copies(outs, j, 10, False):
                one.wait()

    def back_tiles(w, dg_s, du_s, h_s, dy_s, dh_s):
        load = pltpu.make_async_copy(gu, w, local.at[8])
        load.start()
        to_y(11)
        load.wait()

        def compute(i):
            back_tile(dg_s[i], du_s[i], h_s[i], dy_s[i], w, dh_s.at[i])

        tiles(((dg, dg_s), (du, du_s), (h, h_s), (dy, dy_s)), ((dh_out, dh_s),), compute, AFTER_BACK)

    def through_tiles(w, dh_s, gate_s, up_s, dg_s, du_s):
        load = pltpu.make_async_copy(wd, w, local.at[8])
        load.start()
        load.wait()

        def compute(i):
            through_tile(dh_s.at[i], gate_s.at[i], up_s.at[i], w, dg_s.at[i], du_s.at[i])

        tiles(((dh_out, dh_s), (gate, gate_s), (up, up_s)), ((dg_out, dg_s), (du_out, du_s)), compute, AFTER_THROUGH)

    pl.run_scoped(products, VMEM((T, FF), BF), VMEM((T, D), BF), VMEM((2, 4 * RG, T), BF), VMEM((2, 4 * PAD, T), BF))
    if more:
        wide_s, wide32_s, thin_s = VMEM((2, TILE, FF), BF), VMEM((2, TILE, FF), WIDE), VMEM((2, TILE, D), BF)
        pl.run_scoped(back_tiles, VMEM((2, D, FF), BF), wide_s, wide_s, thin_s, thin_s, thin_s)
        pl.run_scoped(through_tiles, VMEM((FF, D), BF), thin_s, wide32_s, wide32_s, wide_s, wide_s)
    else:
        to_y(11)
        for q in (6, 8, 7, 9, 10, 11):
            to_z(q)
    for s in range(12):
        if s >= 10:
            by_core(s).wait_send()
        by_y(s).wait_send()
        if ORDER[s % 4]:
            by_z(s).wait_send()


def scatter(ident, hid, a, dy, dg, du, more=()):
    vm = pl.BlockSpec(memory_space=pltpu.VMEM)
    outs = [jax.ShapeDtypeStruct((RG, FF), BF)] * 2 + [jax.ShapeDtypeStruct((RD, D), BF)]
    if more:
        outs += [jax.ShapeDtypeStruct((T, D), BF)] + [jax.ShapeDtypeStruct((T, FF), BF)] * 2
    return pl.pallas_call(
        functools.partial(scatter_kernel, bool(more)),
        in_specs=[ANY] * (5 + len(more)),
        out_specs=[vm] * 3 + ([ANY] * 3 if more else []),
        out_shape=outs,
        scratch_shapes=[
            VMEM((8, 2, RG, FF), BF),
            VMEM((4, 2, RD, D), BF),
            VMEM((8, 2, RG, FF), BF),
            VMEM((4, 2, RD, D), BF),
            VMEM((2, 2, RG, FF), BF),
            VMEM((2, 2, RD, D), BF),
            VMEM((8, RG, FF), BF),
            VMEM((4, RD, D), BF),
            VMEM((6, RG, FF), BF),
            VMEM((3, RD, D), BF),
            pltpu.SemaphoreType.DMA((36,)),
            pltpu.SemaphoreType.DMA((36,)),
            pltpu.SemaphoreType.DMA((10,)),
            pltpu.SemaphoreType.DMA((16,)),
        ],
        compiler_params=pltpu.CompilerParams(collective_id=ident, has_side_effects=True, vmem_limit_bytes=ROOM),
        name="scatter",
    )(hid, a.reshape(16, RG, T), dy, dg, du, *more)


def solution(mesh):
    def step(x, dy, *arrays):
        weights, m, v = (arrays[i : i + 3] for i in (0, 3, 6))
        x, dy = x[0], dy[0]
        full0, down0, full1, down1, gate0, up0, hid0, a0, h1 = forward(x, *weights)
        hid1, a1, dg1, du1 = turn(h1, dy, full1, down1)
        more = (h1, full1.reshape(2, D, FF), down0, gate0, up0)
        gate_g1, up_g1, down_g1, dh1, dg0, du0 = scatter(1, hid1, a1, dy, dg1, du1, more)
        gate_g0, up_g0, down_g0 = scatter(2, hid0, a0, dh1, dg0, du0)
        gradients = [(gate_g0, gate_g1), (up_g0, up_g1), (down_g0, down_g1)]
        new = [
            adamw(w.astype(WIDE), m, v, jnp.stack([one.astype(WIDE) for one in g]))
            for w, m, v, g in zip(weights, m, v, gradients, strict=True)
        ]
        return tuple(one[which] for which in range(3) for one in new)

    states, cut = P(("rep", "dp"), None, None), P(None, "dp", None)
    return jax.shard_map(
        step,
        mesh=mesh,
        in_specs=(states, states) + (cut,) * 9,
        out_specs=(P("rep", "dp", None),) * 9,
        check_vma=False,
    )
```
